32 devices in a mesh: psr: 8 (over z, x), toa: 4 (over y, core).
Axes of the slice: x: 2, y: 2, z: 4, core: 2. Of those that a mesh axis runs over, the one named last changes fastest.
Arguments:
- design: bfloat16 [3072, 128, 256], P(('psr', 'toa')), may hold values from -0.035888672 to 0.035888672
- noise_weight: float32 [3072, 128], P(('psr', 'toa')), may hold values from 0.3 to 3
- residuals: bfloat16 [3072, 128], P(('psr', 'toa')), may hold values from -6 to 6
- slot_pulsar: int32 [3072], P(('psr', 'toa')), may hold values from 0 to 7, as said below
- slot_rows: int32 [3072], P(('psr', 'toa')), may hold values from 0 to 128, as said below
- own_prior: float32 [64, 192], P(('psr', 'toa')), may hold values from 0.2 to 5
- spectrum: float32 [32], replicated, may hold values from 0.05 to 2
- directions: float32 [3, 64], replicated, may hold values from -1 to 1, as said below
Outputs:
- coeffs: float32 [64, 64], P(('psr', 'toa'))
- log_dets: float32 [64], P(('psr', 'toa'))
- chi_square: float32 [64], P(('psr', 'toa'))
The draws below stay inside these ranges and needn't reach their ends.
Inputs may be any that keep to these rules, and one draw needn't show every extreme that they name: `slot_pulsar`: pulsar k of group g is pulsar g * 8 + k of the arrays with a pulsar dimension; empty blocks name pulsar 0. `slot_rows`: on each device the blocks holding TOAs come first and the empty ones (0 rows) last; within a psr group a pulsar's blocks are consecutive in device order, cyclically, all full but its last; every pulsar has between 4 * 96 * 4 and 4 * 96 * 16 TOAs. `directions`: unit vectors; any two are at least 0.1 radians apart.
All inputs are finite; a program needn't handle non-finite values.
Results may differ from the reference program's by a relative error of at most 0.003.
Values sent between devices are 32-bit elements; how exact they have to be, the bound alone decides.
A program may use at most 128 MiB of HBM per device.

```python
import math
import jax
import jax.numpy as jnp
from jax import lax

GROUP_PULSARS = 8
PULSARS = 64
COLUMNS = 256
FREQS = 32
OWN = 192
BLOCK_ROWS = 128
SLOTS = 96
BLOCKS = 3072
ITERS = 8
N_PSR = 8
N_TOA = 4


def slot_layout(key):
    capacity = N_TOA * SLOTS
    pulsar_cap = capacity * BLOCK_ROWS // GROUP_PULSARS
    toa_counts = jax.random.randint(jax.random.fold_in(key, 101), (N_PSR, GROUP_PULSARS), pulsar_cap // 4, pulsar_cap + 1)
    blocks = (toa_counts + BLOCK_ROWS - 1) // BLOCK_ROWS
    block_ends = jnp.cumsum(blocks, axis=1)
    begins = block_ends - blocks
    first_device = jax.random.randint(jax.random.fold_in(key, 102), (N_PSR, 1), 0, N_TOA)
    position = jnp.arange(capacity, dtype=jnp.int32)[None, :]
    group_block = (position - first_device * SLOTS) % capacity
    inside = (group_block[:, :, None] >= begins[:, None, :]) & (group_block[:, :, None] < block_ends[:, None, :])
    serial = jnp.arange(GROUP_PULSARS, dtype=jnp.int32)[None, None, :]
    pulsar = jnp.sum(jnp.where(inside, serial, 0), axis=2)
    filled = jnp.any(inside, axis=2)
    last_block = jnp.sum(jnp.where(inside, (block_ends - 1)[:, None, :], 0), axis=2)
    tail_rows = jnp.sum(jnp.where(inside, (toa_counts - BLOCK_ROWS * (blocks - 1))[:, None, :], 0), axis=2)
    row_count = jnp.where(filled, jnp.where(group_block == last_block, tail_rows, BLOCK_ROWS), 0)
    return (pulsar.reshape(-1).astype(jnp.int32), row_count.reshape(-1).astype(jnp.int32))


def draw_slot_pulsar(key, part):
    return slot_layout(key)[0]


def draw_slot_rows(key, part):
    return slot_layout(key)[1]


def draw_directions(key, part):
    clusters = N_PSR
    members = GROUP_PULSARS
    number = clusters * members
    serial = jnp.arange(clusters).astype(jnp.float32)
    offset_angle = jax.random.uniform(jax.random.fold_in(key, 201), (), jnp.float32, 0.0, 6.2831853)
    height = 1.0 - (2.0 * serial + 1.0) / clusters
    azimuth = 2.39996323 * serial + offset_angle
    radius = jnp.sqrt(jnp.maximum(1.0 - height * height, 0.0))
    centre = jnp.stack([radius * jnp.cos(azimuth), radius * jnp.sin(azimuth), height], axis=1)
    east_axis = jnp.stack([-jnp.sin(azimuth), jnp.cos(azimuth), jnp.zeros_like(azimuth)], axis=1)
    north_axis = jnp.cross(centre, east_axis)
    cycle_size = jax.random.uniform(jax.random.fold_in(key, 202), (clusters, 1), jnp.float32, 0.135, 0.16)
    cycle_turn = jax.random.uniform(jax.random.fold_in(key, 203), (clusters, 1), jnp.float32, 0.0, 6.2831853)
    spoke_shake = jax.random.uniform(jax.random.fold_in(key, 204), (clusters, members), jnp.float32, -0.03, 0.03)
    radial_shake = jax.random.uniform(jax.random.fold_in(key, 205), (clusters, members), jnp.float32, 0.97, 1.03)
    member_index = jnp.arange(members).astype(jnp.float32)[None, :]
    spoke_angle = 6.2831853 * (member_index - 1.0) / (members - 1) + cycle_turn + spoke_shake
    distance = jnp.where(member_index > 0.5, cycle_size * radial_shake, 0.0)
    across = jnp.cos(spoke_angle)[:, :, None] * east_axis[:, None, :] + jnp.sin(spoke_angle)[:, :, None] * north_axis[:, None, :]
    points = jnp.cos(distance)[:, :, None] * centre[:, None, :] + jnp.sin(distance)[:, :, None] * across
    points = points.reshape((number, 3)).T
    shuffle = jax.random.permutation(jax.random.fold_in(key, 206), number)
    return points[:, shuffle].astype(jnp.float32)


def levels(rng, extent, split, smallest, largest):
    factor_of, own = 1.0, jax.random.fold_in(rng, 6)
    for axis_at, parts in split:
        draws = jnp.exp(jax.random.uniform(jax.random.fold_in(own, axis_at), (parts,), jnp.float32, smallest / len(split), largest / len(split)))
        factor_of = factor_of * jnp.repeat(draws, extent[axis_at] // parts).reshape([-1 if axis == axis_at else 1 for axis in range(len(extent))])
    return factor_of


def bell_draw(stream_key, dims, deviation, bound, cuts=(), held_as=jnp.bfloat16):
    level = levels(stream_key, dims, cuts, -0.22, 0.18) if cuts else 1.0
    array = jax.random.normal(stream_key, dims, jnp.float32) * deviation * level
    return jnp.minimum(jnp.maximum(array, -bound), bound).astype(held_as)


def setup_inputs(seed: int = 0) -> dict:
    keys = jax.random.split(jax.random.key(seed), 9)
    return {
        "design": bell_draw(keys[0], (BLOCKS, BLOCK_ROWS, COLUMNS), 0.006, 0.035888672, ((0, 32),)),
        "noise_weight": jnp.clip(jnp.exp(math.log(3.0) - 2.3025851 * jax.random.uniform(keys[1], (BLOCKS, BLOCK_ROWS), jnp.float32) ** levels(keys[1], (BLOCKS, BLOCK_ROWS), ((0, 32),), -0.2, 0.2)), 0.3, 3.0),
        "residuals": bell_draw(keys[2], (BLOCKS, BLOCK_ROWS), 1.0, 6.0, ((0, 32),)),
        "slot_pulsar": draw_slot_pulsar(jax.random.fold_in(keys[8], 71), 0),
        "slot_rows": draw_slot_rows(jax.random.fold_in(keys[8], 71), 0),
        "own_prior": jnp.clip(jnp.exp(math.log(5.0) - 3.218876 * jax.random.uniform(keys[5], (PULSARS, OWN), jnp.float32) ** levels(keys[5], (PULSARS, OWN), ((0, 32),), -0.2, 0.2)), 0.2, 5.0),
        "spectrum": jnp.clip(jnp.exp(jax.random.uniform(keys[6], (FREQS,), jnp.float32, math.log(0.05), math.log(2.0))), 0.05, 2.0),
        "directions": draw_directions(jax.random.fold_in(keys[8], 71), 0),
    }


highest = lax.Precision.HIGHEST

def cholesky_solve(factor, right_side):
    halfway = lax.linalg.triangular_solve(factor, right_side, left_side=True, lower=True)
    return lax.linalg.triangular_solve(factor, halfway, left_side=True, lower=True, transpose_a=True)

def slot_term_values(design, weight, residuals, pulsar, slot_rows):
    positions = lax.broadcasted_iota(jnp.int32, weight.shape, 1)
    weight = jnp.where(positions < slot_rows[:, None], weight, 0.0)
    weighted = (weight[:, :, None] * design.astype(jnp.float32)).astype(jnp.bfloat16)
    weighted = lax.optimization_barrier(weighted)
    wide_weighted = weighted.astype(jnp.float32)
    wide_design = design.astype(jnp.float32)
    wide_residual = residuals.astype(jnp.float32)
    products = jnp.einsum('srk,srl->skl', wide_weighted, wide_design, precision=highest)
    fitted = jnp.einsum('srk,sr->sk', wide_weighted, wide_residual, precision=highest)
    energy = jnp.sum(weight * wide_residual * wide_residual, axis=1)
    owners = (pulsar[:, None] == lax.broadcasted_iota(jnp.int32, (pulsar.shape[0], GROUP_PULSARS), 1)).astype(jnp.float32)
    return (jnp.einsum('sp,skl->pkl', owners, products, precision=highest), jnp.einsum('sp,sk->pk', owners, fitted, precision=highest), jnp.dot(energy, owners, precision=highest), jnp.dot(slot_rows.astype(jnp.float32), owners, precision=highest))

def group_grams(design, weight, residuals, pulsar, slot_rows):
    count_blocks = design.shape[0] // 16
    column_count = design.shape[2]

    def regroup(member):
        return member.reshape((count_blocks, 16) + member.shape[1:])

    def one_block(running_total, group_members):
        summand_terms = slot_term_values(*group_members)
        return (tuple((earlier_term + later_term for earlier_term, later_term in zip(running_total, summand_terms))), 0)
    initial = (jnp.zeros((GROUP_PULSARS, column_count, column_count), jnp.float32), jnp.zeros((GROUP_PULSARS, column_count), jnp.float32), jnp.zeros((GROUP_PULSARS,), jnp.float32), jnp.zeros((GROUP_PULSARS,), jnp.float32))
    group_members = tuple((regroup(member) for member in (design, weight, residuals, pulsar, slot_rows)))
    totals, unused = lax.scan(one_block, initial, group_members)
    return totals

def eliminate(gram_sums, projections, own_prior):
    column_count = gram_sums.shape[1]
    common = column_count - own_prior.shape[1]
    identity = jnp.eye(own_prior.shape[1], dtype=jnp.float32)
    own_block = gram_sums[:, common:, common:] + (1.0 / own_prior)[:, :, None] * identity[None, :, :]
    factor = jnp.linalg.cholesky(own_block)
    right_side = jnp.concatenate([gram_sums[:, common:, :common], projections[:, common:, None]], axis=2)
    solved = cholesky_solve(factor, right_side)
    cross_block = gram_sums[:, :common, common:]
    reduced = jnp.einsum('pck,pkd->pcd', cross_block, solved, precision=highest)
    schur_part = gram_sums[:, :common, :common] - reduced[:, :, :common]
    target = projections[:, :common] - reduced[:, :, common]
    quadratic = jnp.sum(projections[:, common:] * solved[:, :, common], axis=1)
    own_logdet = 2.0 * jnp.sum(jnp.log(jnp.diagonal(factor, axis1=1, axis2=2)), axis=1)
    return (schur_part, target, quadratic, own_logdet)

def coupling_inverse(directions):
    cosines = jnp.clip(jnp.dot(directions.T, directions, precision=highest), -1.0, 1.0)
    number = cosines.shape[0]
    diagonal = jnp.eye(number, dtype=jnp.float32) > 0.5
    spread = jnp.where(diagonal, 1.0, 0.5 * (1.0 - cosines))
    intersect_curve = 1.5 * spread * jnp.log(spread) - 0.25 * spread + 0.5
    correlation = jnp.where(diagonal, 1.0, intersect_curve)
    factor = jnp.linalg.cholesky(correlation)
    return cholesky_solve(factor, jnp.eye(number, dtype=jnp.float32))

def coupled_apply(schur_part, coupling, inverse_power, vector):
    within = jnp.einsum('pcd,pd->pc', schur_part, vector, precision=highest)
    mixing = jnp.dot(coupling, vector, precision=highest)
    return within + mixing * inverse_power[None, :]

def precondition(block_factor, residual):
    return cholesky_solve(block_factor, residual[:, :, None])[:, :, 0]

def reference(design, noise_weight, residuals, slot_pulsar, slot_rows, own_prior, spectrum, directions):
    groups = N_PSR
    group_slots = design.shape[0] // groups
    shaped = tuple((member.reshape((groups, group_slots) + member.shape[1:]) for member in (design, noise_weight, residuals, slot_pulsar, slot_rows)))

    def per_group(group_members):
        return group_grams(*group_members)
    gram_sums, projections, energy, counts = lax.map(per_group, shaped)
    gram_sums = gram_sums.reshape((PULSARS, COLUMNS, COLUMNS))
    projections = projections.reshape((PULSARS, COLUMNS))
    energy = energy.reshape((PULSARS,))
    counts = counts.reshape((PULSARS,))
    schur_part, target, quadratic, own_logdet = eliminate(gram_sums, projections, own_prior)
    coupling = coupling_inverse(directions)
    inverse_power = 1.0 / jnp.repeat(spectrum, 2)
    block_matrix = schur_part + jnp.diagonal(coupling)[:, None, None] * jnp.diag(inverse_power)[None, :, :]
    block_factor = jnp.linalg.cholesky(block_matrix)
    block_logdet = 2.0 * jnp.sum(jnp.log(jnp.diagonal(block_factor, axis1=1, axis2=2)), axis=1)
    solution = jnp.zeros_like(target)
    residual = target
    scaled = precondition(block_factor, residual)
    direction = scaled
    inner_now = jnp.sum(residual * scaled)
    for iteration in range(ITERS):
        mapped = coupled_apply(schur_part, coupling, inverse_power, direction)
        step_size = inner_now / jnp.sum(direction * mapped)
        solution = solution + step_size * direction
        residual = residual - step_size * mapped
        if iteration + 1 < ITERS:
            scaled = precondition(block_factor, residual)
            inner_next = jnp.sum(residual * scaled)
            direction = scaled + inner_next / inner_now * direction
            inner_now = inner_next
    log_dets = (own_logdet + block_logdet) / COLUMNS
    chi_square = (energy - quadratic - jnp.sum(target * solution, axis=1)) / counts
    return (solution, log_dets, chi_square)
```

```python
import functools

import jax
import jax.numpy as jnp
from jax import lax
from jax.experimental import pallas as pl
from jax.experimental.pallas import tpu as pltpu
from jax.sharding import PartitionSpec as P

GROUP_PULSARS = 8
ITERS = 8
SIDE = 64
STEP_SLOTS = 8
highest = lax.Precision.HIGHEST


def dot(a, b, precision=highest):
    return jnp.dot(a, b, precision=precision, preferred_element_type=jnp.float32)


def gram_kernel(pulsar_ref, rows_ref, design_ref, weight_ref, residual_ref, out_ref):
    step = pl.program_id(0)
    toas, columns = design_ref.shape[1], design_ref.shape[2]

    @pl.when(step == 0)
    def _():
        out_ref[...] = jnp.zeros_like(out_ref)

    lanes = lax.broadcasted_iota(jnp.int32, (1, toas), 1)
    for j in range(STEP_SLOTS):
        slot = step * STEP_SLOTS + j
        p = pulsar_ref[slot]
        valid = lanes < rows_ref[slot]
        weight = jnp.where(valid, weight_ref[j : j + 1, :], 0.0)
        residual = residual_ref[j : j + 1, :].astype(jnp.float32)
        block = design_ref[j]
        across = jnp.transpose(block).astype(jnp.float32)
        weighted = (across * weight).astype(jnp.bfloat16)
        gram = jnp.dot(weighted, block, preferred_element_type=jnp.float32)
        spread = jnp.broadcast_to(residual, (8, toas)).astype(jnp.bfloat16)
        fitted = lax.dot_general(
            spread, weighted, (((1,), (1,)), ((), ())), preferred_element_type=jnp.float32
        )
        energy = weight * residual * residual
        count = jnp.where(valid, 1.0, 0.0)
        tail = jnp.concatenate([energy, count], axis=1)
        at_row = lax.broadcasted_iota(jnp.int32, (8, columns), 0)
        extra = jnp.where(at_row == 0, fitted, jnp.where(at_row == 1, tail, 0.0))
        out_ref[p, 0:columns, :] += gram
        out_ref[p, columns : columns + 8, :] += extra


def local_grams(design, noise_weight, residuals, slot_pulsar, slot_rows):
    slots, toas, columns = design.shape
    return pl.pallas_call(
        gram_kernel,
        grid_spec=pltpu.PrefetchScalarGridSpec(
            num_scalar_prefetch=2,
            grid=(slots // STEP_SLOTS,),
            in_specs=[
                pl.BlockSpec((STEP_SLOTS, toas, columns), lambda i, *_: (i, 0, 0)),
                pl.BlockSpec((STEP_SLOTS, toas), lambda i, *_: (i, 0)),
                pl.BlockSpec((STEP_SLOTS, toas), lambda i, *_: (i, 0)),
            ],
            out_specs=pl.BlockSpec((GROUP_PULSARS, columns + 8, columns), lambda i, *_: (0, 0, 0)),
        ),
        out_shape=jax.ShapeDtypeStruct((GROUP_PULSARS, columns + 8, columns), jnp.float32),
        name="gram",
    )(slot_pulsar, slot_rows, design, noise_weight, residuals)


def invert(mats):
    side = mats[0].shape[0]
    lane = lax.broadcasted_iota(jnp.int32, (1, side), 1)
    sub = lax.broadcasted_iota(jnp.int32, (side, side), 0)
    lane_full = lax.broadcasted_iota(jnp.int32, (side, side), 1)
    pivots = [jnp.ones((1, side), jnp.float32) for _ in mats]
    mats = list(mats)
    for k in range(side):
        for m, a in enumerate(mats):
            row = a[k : k + 1, :]
            col = a[:, k : k + 1]
            pivot = a[k : k + 1, k : k + 1]
            inverse = 1.0 / pivot
            pivots[m] = jnp.where(lane == k, pivot, pivots[m])
            row = jnp.where(lane == k, 1.0, row) * inverse
            kept = jnp.where(lane_full == k, 0.0, a)
            mats[m] = jnp.where(sub == k, row, kept - col * row)
    return mats, [jnp.sum(jnp.log(v), axis=1, keepdims=True) for v in pivots]


def coupling_kernel(directions_ref, out_ref):
    d = directions_ref[...]
    cosines = jnp.clip(
        lax.dot_general(d, d, (((0,), (0,)), ((), ())), precision=highest, preferred_element_type=jnp.float32),
        -1.0,
        1.0,
    )
    number = cosines.shape[0]
    row = lax.broadcasted_iota(jnp.int32, (number, number), 0)
    col = lax.broadcasted_iota(jnp.int32, (number, number), 1)
    spread = jnp.where(row == col, 1.0, 0.5 * (1.0 - cosines))
    curve = 1.5 * spread * jnp.log(spread) - 0.25 * spread + 0.5
    x = jnp.where(row == col, 1.0, curve)
    side = min(SIDE, number)
    for b in range(number // side):
        lo, hi = b * side, (b + 1) * side
        (inverse,), _ = invert([x[lo:hi, lo:hi]])
        if number == side:
            x = inverse
            continue
        across = dot(inverse, x[lo:hi, :])
        down = x[:, lo:hi]
        inside_row = (row >= lo) & (row < hi)
        inside_col = (col >= lo) & (col < hi)
        updated = x - dot(down, across)
        placed = -dot(down, inverse)
        tiles = number // side
        updated = jnp.where(inside_col, jnp.concatenate([placed] * tiles, axis=1), updated)
        fixed = jnp.where(inside_col, jnp.concatenate([jnp.concatenate([inverse] * tiles, axis=1)] * tiles, axis=0),
                          jnp.concatenate([across] * tiles, axis=0))
        x = jnp.where(inside_row, fixed, updated)
    out_ref[...] = x


def coupling_inverse(directions):
    number = directions.shape[1]
    padded = jnp.pad(directions, ((0, 8 - directions.shape[0]), (0, 0)))
    return pl.pallas_call(
        coupling_kernel,
        out_shape=jax.ShapeDtypeStruct((number, number), jnp.float32),
        cost_estimate=pl.CostEstimate(flops=number**3 * 60, bytes_accessed=4 * number * number, transcendentals=0),
        name="coupling",
    )(padded)


def eliminate_kernel(toa_devices, sums_ref, prior_ref, coupling_ref, power_ref, packed_ref, extra_ref, work_ref):
    owned, height, columns = sums_ref.shape
    common = columns - prior_ref.shape[2]
    device = lax.axis_index("psr") * toa_devices + lax.axis_index("toa")
    row = lax.broadcasted_iota(jnp.int32, (height, columns), 0)
    col = lax.broadcasted_iota(jnp.int32, (height, columns), 1)
    energies, counts = [], []
    for i in range(owned):
        diag = jnp.concatenate([jnp.zeros((1, common), jnp.float32), 1.0 / prior_ref[i]], axis=1)
        tail = sums_ref[i, columns + 1 : columns + 2, :]
        energies.append(jnp.sum(tail[:, : columns // 2], axis=1, keepdims=True))
        counts.append(jnp.sum(tail[:, columns // 2 :], axis=1, keepdims=True))
        work_ref[i] = sums_ref[i] + jnp.where(row == col, diag, 0.0)
    logs = [jnp.zeros((1, 1), jnp.float32)] * owned
    quads = [jnp.zeros((1, 1), jnp.float32)] * owned
    for lo in range(common, columns, SIDE):
        hi = lo + SIDE
        inverses, extra_logs = invert([work_ref[i, lo:hi, lo:hi] for i in range(owned)])
        for i in range(owned):
            logs[i] = logs[i] + extra_logs[i]
            down = work_ref[i, :, lo:hi]
            scaled = dot(down, inverses[i])
            quads[i] = quads[i] + jnp.sum(
                scaled[columns : columns + 1] * down[columns : columns + 1], axis=1, keepdims=True
            )
            work_ref[i] = work_ref[i] - dot(scaled, work_ref[i, lo:hi, :])
    lane_p = lax.broadcasted_iota(jnp.int32, (1, coupling_ref.shape[1]), 1)
    rc = lax.broadcasted_iota(jnp.int32, (common, common), 0)
    cc = lax.broadcasted_iota(jnp.int32, (common, common), 1)
    blocks = []
    for i in range(owned):
        p = device * owned + i
        own = jnp.sum(jnp.where(lane_p == p, coupling_ref[pl.ds(p, 1), :], 0.0), axis=1, keepdims=True)
        blocks.append(work_ref[i, :common, :common] + jnp.where(rc == cc, own * power_ref[...], 0.0))
    inverses, block_logs = invert(blocks)
    half = common // 2
    lane = lax.broadcasted_iota(jnp.int32, (1, 128 - common), 1)
    for i in range(owned):
        packed_ref[i, 0:half, :] = jnp.concatenate([inverses[i][:half], inverses[i][half:]], axis=1)
        target = work_ref[i, columns : columns + 1, :common]
        facts = jnp.where(lane == 0, (logs[i] + block_logs[i]) / columns, 0.0)
        facts = jnp.where(lane == 1, energies[i] - quads[i], facts)
        facts = jnp.where(lane == 2, counts[i], facts)
        line = jnp.concatenate([target, facts], axis=1)
        packed_ref[i, half : half + 8, :] = jnp.broadcast_to(line, (8, 128))
        extra_ref[i : i + 1, :] = line


def eliminate(sums, own_prior, coupling, power, toa_devices):
    owned, height, columns = sums.shape
    common = columns - own_prior.shape[1]
    return pl.pallas_call(
        functools.partial(eliminate_kernel, toa_devices),
        out_shape=(
            jax.ShapeDtypeStruct((owned, common // 2 + 8, 2 * common), jnp.float32),
            jax.ShapeDtypeStruct((owned, 2 * common), jnp.float32),
        ),
        scratch_shapes=[pltpu.VMEM((owned, height, columns), jnp.float32)],
        name="eliminate",
    )(sums, own_prior[:, None, :], coupling, power)


def conjugate_kernel(packed_ref, coupling_ref, power_ref, out_ref, blocks_ref, w_ref):
    number = coupling_ref.shape[0]
    common = power_ref.shape[0]
    half = common // 2
    stride = half + 8

    def spread(k, carry):
        x = jnp.transpose(packed_ref[pl.ds(k, number, stride=stride), :])
        blocks_ref[k] = x[:common]
        blocks_ref[k + half] = x[common:]
        return carry

    lax.fori_loop(0, half, spread, 0)
    target = jnp.transpose(packed_ref[pl.ds(half, number, stride=stride), :])[:common]
    row = lax.broadcasted_iota(jnp.int32, (number, number), 0)
    col = lax.broadcasted_iota(jnp.int32, (number, number), 1)
    mixing = jnp.where(row == col, 0.0, coupling_ref[...])
    power = power_ref[...]

    def total(x):
        return jnp.sum(jnp.sum(x, axis=0, keepdims=True), axis=1, keepdims=True)

    def apply_blocks(v):
        w_ref[...] = v
        acc = jnp.zeros((common, number), jnp.float32)
        for k in range(common):
            acc = acc + blocks_ref[k] * w_ref[k : k + 1, :]
        return acc

    solution = jnp.zeros((common, number), jnp.float32)
    residual = target
    scaled = apply_blocks(residual)
    direction, block_direction = scaled, residual
    inner = total(residual * scaled)
    for iteration in range(ITERS):
        coupled = power * dot(direction, mixing)
        mapped = block_direction + coupled
        step = inner / total(direction * mapped)
        solution = solution + step * direction
        if iteration + 1 < ITERS:
            residual = residual - step * mapped
            scaled = scaled - step * (direction + apply_blocks(coupled))
            following = total(residual * scaled)
            ratio = following / inner
            direction = scaled + ratio * direction
            block_direction = residual + ratio * block_direction
            inner = following
    out_ref[...] = jnp.transpose(solution)


def conjugate(packed, coupling, power):
    number = coupling.shape[0]
    common = power.shape[0]
    return pl.pallas_call(
        conjugate_kernel,
        out_shape=jax.ShapeDtypeStruct((number, common), jnp.float32),
        scratch_shapes=[
            pltpu.VMEM((common, common, number), jnp.float32),
            pltpu.VMEM((common, number), jnp.float32),
        ],
        name="conjugate",
    )(packed.reshape(-1, packed.shape[-1]), coupling, power)


def body(design, noise_weight, residuals, slot_pulsar, slot_rows, own_prior, spectrum, directions):
    toa_devices = lax.axis_size("toa")
    owned = GROUP_PULSARS // toa_devices
    device = lax.axis_index("psr") * toa_devices + lax.axis_index("toa")
    partial = local_grams(design, noise_weight, residuals, slot_pulsar, slot_rows)
    sums = lax.psum_scatter(partial, "toa", scatter_dimension=0, tiled=True)
    coupling = coupling_inverse(directions)
    power = 1.0 / jnp.repeat(spectrum, 2)
    packed, extra = eliminate(sums, own_prior, coupling, power[None, :], toa_devices)
    everything = lax.all_gather(packed, ("psr", "toa"), axis=0, tiled=True)
    whole = conjugate(everything, coupling, power[:, None])
    common = whole.shape[1]
    solution = lax.dynamic_slice_in_dim(whole, device * owned, owned, 0)
    chi_square = (extra[:, common + 1] - jnp.sum(extra[:, :common] * solution, axis=1)) / extra[:, common + 2]
    return (solution, extra[:, common], chi_square)


def solution(mesh):
    return jax.shard_map(
        body,
        mesh=mesh,
        in_specs=(
            P(("psr", "toa"), None, None),
            P(("psr", "toa"), None),
            P(("psr", "toa"), None),
            P(("psr", "toa")),
            P(("psr", "toa")),
            P(("psr", "toa"), None),
            P(),
            P(),
        ),
        out_specs=(P(("psr", "toa"), None), P(("psr", "toa")), P(("psr", "toa"))),
        check_vma=False,
    )
```

```python
import functools

import jax
import jax.numpy as jnp
from jax import lax
from jax.experimental import pallas as pl
from jax.experimental.pallas import tpu as pltpu
from jax.sharding import PartitionSpec as P

GROUP_PULSARS = 8
ITERS = 8
SIDE = 64
STEP_SLOTS = 8
highest = lax.Precision.HIGHEST


def dot(a, b, precision=highest):
    return jnp.dot(a, b, precision=precision, preferred_element_type=jnp.float32)


def gram_kernel(pulsar_ref, rows_ref, design_ref, weight_ref, residual_ref, out_ref):
    step = pl.program_id(0)
    toas, columns = design_ref.shape[1], design_ref.shape[2]

    @pl.when(step == 0)
    def _():
        out_ref[...] = jnp.zeros_like(out_ref)

    lanes = lax.broadcasted_iota(jnp.int32, (1, toas), 1)
    for j in range(STEP_SLOTS):
        slot = step * STEP_SLOTS + j
        p = pulsar_ref[slot]
        valid = lanes < rows_ref[slot]
        weight = jnp.where(valid, weight_ref[j : j + 1, :], 0.0)
        residual = residual_ref[j : j + 1, :].astype(jnp.float32)
        block = design_ref[j]
        across = jnp.transpose(block).astype(jnp.float32)
        weighted = (across * weight).astype(jnp.bfloat16)
        gram = jnp.dot(weighted, block, preferred_element_type=jnp.float32)
        spread = jnp.broadcast_to(residual, (8, toas)).astype(jnp.bfloat16)
        fitted = lax.dot_general(
            spread, weighted, (((1,), (1,)), ((), ())), preferred_element_type=jnp.float32
        )
        energy = weight * residual * residual
        count = jnp.where(valid, 1.0, 0.0)
        tail = jnp.concatenate([energy, count], axis=1)
        at_row = lax.broadcasted_iota(jnp.int32, (8, columns), 0)
        extra = jnp.where(at_row == 0, fitted, jnp.where(at_row == 1, tail, 0.0))
        out_ref[p, 0:columns, :] += gram
        out_ref[p, columns : columns + 8, :] += extra


def local_grams(design, noise_weight, residuals, slot_pulsar, slot_rows):
    slots, toas, columns = design.shape
    return pl.pallas_call(
        gram_kernel,
        grid_spec=pltpu.PrefetchScalarGridSpec(
            num_scalar_prefetch=2,
            grid=(slots // STEP_SLOTS,),
            in_specs=[
                pl.BlockSpec((STEP_SLOTS, toas, columns), lambda i, *_: (i, 0, 0)),
                pl.BlockSpec((STEP_SLOTS, toas), lambda i, *_: (i, 0)),
                pl.BlockSpec((STEP_SLOTS, toas), lambda i, *_: (i, 0)),
            ],
            out_specs=pl.BlockSpec((GROUP_PULSARS, columns + 8, columns), lambda i, *_: (0, 0, 0)),
        ),
        out_shape=jax.ShapeDtypeStruct((GROUP_PULSARS, columns + 8, columns), jnp.float32),
        name="gram",
    )(slot_pulsar, slot_rows, design, noise_weight, residuals)


def invert(mats):
    side = mats[0].shape[0]
    lane = lax.broadcasted_iota(jnp.int32, (1, side), 1)
    sub = lax.broadcasted_iota(jnp.int32, (side, side), 0)
    lane_full = lax.broadcasted_iota(jnp.int32, (side, side), 1)
    pivots = [jnp.ones((1, side), jnp.float32) for _ in mats]
    mats = list(mats)
    for k in range(side):
        for m, a in enumerate(mats):
            row = a[k : k + 1, :]
            col = a[:, k : k + 1]
            pivot = a[k : k + 1, k : k + 1]
            inverse = 1.0 / pivot
            pivots[m] = jnp.where(lane == k, pivot, pivots[m])
            row = jnp.where(lane == k, 1.0, row) * inverse
            kept = jnp.where(lane_full == k, 0.0, a)
            mats[m] = jnp.where(sub == k, row, kept - col * row)
    return mats, [jnp.sum(jnp.log(v), axis=1, keepdims=True) for v in pivots]


def coupling_kernel(directions_ref, out_ref):
    d = directions_ref[...]
    cosines = jnp.clip(
        lax.dot_general(d, d, (((0,), (0,)), ((), ())), precision=highest, preferred_element_type=jnp.float32),
        -1.0,
        1.0,
    )
    number = cosines.shape[0]
    row = lax.broadcasted_iota(jnp.int32, (number, number), 0)
    col = lax.broadcasted_iota(jnp.int32, (number, number), 1)
    spread = jnp.where(row == col, 1.0, 0.5 * (1.0 - cosines))
    curve = 1.5 * spread * jnp.log(spread) - 0.25 * spread + 0.5
    x = jnp.where(row == col, 1.0, curve)
    side = min(SIDE, number)
    for b in range(number // side):
        lo, hi = b * side, (b + 1) * side
        (inverse,), _ = invert([x[lo:hi, lo:hi]])
        if number == side:
            x = inverse
            continue
        across = dot(inverse, x[lo:hi, :])
        down = x[:, lo:hi]
        inside_row = (row >= lo) & (row < hi)
        inside_col = (col >= lo) & (col < hi)
        updated = x - dot(down, across)
        placed = -dot(down, inverse)
        tiles = number // side
        updated = jnp.where(inside_col, jnp.concatenate([placed] * tiles, axis=1), updated)
        fixed = jnp.where(inside_col, jnp.concatenate([jnp.concatenate([inverse] * tiles, axis=1)] * tiles, axis=0),
                          jnp.concatenate([across] * tiles, axis=0))
        x = jnp.where(inside_row, fixed, updated)
    out_ref[...] = x


def coupling_inverse(directions):
    number = directions.shape[1]
    padded = jnp.pad(directions, ((0, 8 - directions.shape[0]), (0, 0)))
    return pl.pallas_call(
        coupling_kernel,
        out_shape=jax.ShapeDtypeStruct((number, number), jnp.float32),
        cost_estimate=pl.CostEstimate(flops=number**3 * 60, bytes_accessed=4 * number * number, transcendentals=0),
        name="coupling",
    )(padded)


def eliminate_kernel(toa_devices, sums_ref, prior_ref, coupling_ref, power_ref, packed_ref, extra_ref, work_ref):
    owned, height, columns = sums_ref.shape
    common = columns - prior_ref.shape[2]
    device = lax.axis_index("psr") * toa_devices + lax.axis_index("toa")
    row = lax.broadcasted_iota(jnp.int32, (height, columns), 0)
    col = lax.broadcasted_iota(jnp.int32, (height, columns), 1)
    energies, counts = [], []
    for i in range(owned):
        diag = jnp.concatenate([jnp.zeros((1, common), jnp.float32), 1.0 / prior_ref[i]], axis=1)
        tail = sums_ref[i, columns + 1 : columns + 2, :]
        energies.append(jnp.sum(tail[:, : columns // 2], axis=1, keepdims=True))
        counts.append(jnp.sum(tail[:, columns // 2 :], axis=1, keepdims=True))
        work_ref[i] = sums_ref[i] + jnp.where(row == col, diag, 0.0)
    logs = [jnp.zeros((1, 1), jnp.float32)] * owned
    quads = [jnp.zeros((1, 1), jnp.float32)] * owned
    for lo in range(common, columns, SIDE):
        hi = lo + SIDE
        inverses, extra_logs = invert([work_ref[i, lo:hi, lo:hi] for i in range(owned)])
        for i in range(owned):
            logs[i] = logs[i] + extra_logs[i]
            down = work_ref[i, :, lo:hi]
            scaled = dot(down, inverses[i])
            quads[i] = quads[i] + jnp.sum(
                scaled[columns : columns + 1] * down[columns : columns + 1], axis=1, keepdims=True
            )
            work_ref[i] = work_ref[i] - dot(scaled, work_ref[i, lo:hi, :])
    lane_p = lax.broadcasted_iota(jnp.int32, (1, coupling_ref.shape[1]), 1)
    rc = lax.broadcasted_iota(jnp.int32, (common, common), 0)
    cc = lax.broadcasted_iota(jnp.int32, (common, common), 1)
    blocks = []
    for i in range(owned):
        p = device * owned + i
        own = jnp.sum(jnp.where(lane_p == p, coupling_ref[pl.ds(p, 1), :], 0.0), axis=1, keepdims=True)
        blocks.append(work_ref[i, :common, :common] + jnp.where(rc == cc, own * power_ref[...], 0.0))
    inverses, block_logs = invert(blocks)
    half = common // 2
    lane = lax.broadcasted_iota(jnp.int32, (1, 128 - common), 1)
    for i in range(owned):
        packed_ref[i, 0:half, :] = jnp.concatenate([inverses[i][:half], inverses[i][half:]], axis=1)
        target = work_ref[i, columns : columns + 1, :common]
        facts = jnp.where(lane == 0, (logs[i] + block_logs[i]) / columns, 0.0)
        facts = jnp.where(lane == 1, energies[i] - quads[i], facts)
        facts = jnp.where(lane == 2, counts[i], facts)
        line = jnp.concatenate([target, facts], axis=1)
        packed_ref[i, half : half + 8, :] = jnp.broadcast_to(line, (8, 128))
        extra_ref[i : i + 1, :] = line


def eliminate(sums, own_prior, coupling, power, toa_devices):
    owned, height, columns = sums.shape
    common = columns - own_prior.shape[1]
    return pl.pallas_call(
        functools.partial(eliminate_kernel, toa_devices),
        out_shape=(
            jax.ShapeDtypeStruct((owned, common // 2 + 8, 2 * common), jnp.float32),
            jax.ShapeDtypeStruct((owned, 2 * common), jnp.float32),
        ),
        scratch_shapes=[pltpu.VMEM((owned, height, columns), jnp.float32)],
        name="eliminate",
    )(sums, own_prior[:, None, :], coupling, power)


def conjugate_kernel(packed_ref, coupling_ref, power_ref, out_ref, blocks_ref, w_ref):
    number = coupling_ref.shape[0]
    common = power_ref.shape[0]
    half = common // 2
    stride = half + 8

    def spread(k, carry):
        x = jnp.transpose(packed_ref[pl.ds(k, number, stride=stride), :])
        blocks_ref[k] = x[:common]
        blocks_ref[k + half] = x[common:]
        return carry

    lax.fori_loop(0, half, spread, 0)
    target = jnp.transpose(packed_ref[pl.ds(half, number, stride=stride), :])[:common]
    row = lax.broadcasted_iota(jnp.int32, (number, number), 0)
    col = lax.broadcasted_iota(jnp.int32, (number, number), 1)
    mixing = jnp.where(row == col, 0.0, coupling_ref[...])
    power = power_ref[...]

    def total(x):
        return jnp.sum(jnp.sum(x, axis=0, keepdims=True), axis=1, keepdims=True)

    def apply_blocks(v):
        w_ref[...] = v
        acc = jnp.zeros((common, number), jnp.float32)
        for k in range(common):
            acc = acc + blocks_ref[k] * w_ref[k : k + 1, :]
        return acc

    solution = jnp.zeros((common, number), jnp.float32)
    residual = target
    scaled = apply_blocks(residual)
    direction, block_direction = scaled, residual
    inner = total(residual * scaled)
    for iteration in range(ITERS):
        coupled = power * dot(direction, mixing)
        mapped = block_direction + coupled
        step = inner / total(direction * mapped)
        solution = solution + step * direction
        if iteration + 1 < ITERS:
            residual = residual - step * mapped
            scaled = scaled - step * (direction + apply_blocks(coupled))
            following = total(residual * scaled)
            ratio = following / inner
            direction = scaled + ratio * direction
            block_direction = residual + ratio * block_direction
            inner = following
    out_ref[...] = jnp.transpose(solution)


def conjugate(packed, coupling, power):
    number = coupling.shape[0]
    common = power.shape[0]
    return pl.pallas_call(
        conjugate_kernel,
        out_shape=jax.ShapeDtypeStruct((number, common), jnp.float32),
        scratch_shapes=[
            pltpu.VMEM((common, common, number), jnp.float32),
            pltpu.VMEM((common, number), jnp.float32),
        ],
        name="conjugate",
    )(packed.reshape(-1, packed.shape[-1]), coupling, power)


MESH = pl.DeviceIdType.MESH


def reduce_kernel(chips, partial_ref, out_ref, near_ref, sum_ref, far_ref, near_send, near_recv, far_send, far_recv):
    me = lax.axis_index("toa")
    core = lax.rem(me, 2)
    chip = me // 2
    other = 1 - core
    owned = out_ref.shape[0]
    barrier = pltpu.get_barrier_semaphore()
    pl.semaphore_signal(barrier, inc=1, device_id={"toa": chip * 2 + other}, device_id_type=MESH)
    for d in range(1, chips):
        target = lax.rem(chip + d, chips) * 2 + core
        pl.semaphore_signal(barrier, inc=1, device_id={"toa": target}, device_id_type=MESH)
    pl.semaphore_wait(barrier, chips)
    order = [d % chips for d in range(1, chips + 1)]
    near, far = {}, {}
    for d in order:
        owner = lax.rem(chip + d, chips) * 2 + other
        for i in range(owned):
            near[d, i] = pltpu.make_async_remote_copy(
                src_ref=partial_ref.at[owner * owned + i],
                dst_ref=near_ref.at[d * owned + i],
                send_sem=near_send.at[d * owned + i],
                recv_sem=near_recv.at[d * owned + i],
                device_id={"toa": chip * 2 + other},
                device_id_type=MESH,
            )
            near[d, i].start()
    for d in order:
        owner = lax.rem(chip + d, chips) * 2 + core
        for i in range(owned):
            at = d * owned + i
            near[d, i].wait_recv()
            both = partial_ref[owner * owned + i] + near_ref[at]
            if d == 0:
                out_ref[i] = both
                continue
            sum_ref[at - owned] = both
            far[d, i] = pltpu.make_async_remote_copy(
                src_ref=sum_ref.at[at - owned],
                dst_ref=far_ref.at[at - owned],
                send_sem=far_send.at[at - owned],
                recv_sem=far_recv.at[at - owned],
                device_id={"toa": owner},
                device_id_type=MESH,
            )
            far[d, i].start()
    for (d, i), copy in far.items():
        copy.wait_recv()
        out_ref[i] += far_ref[d * owned + i - owned]
    for copy in list(near.values()) + list(far.values()):
        copy.wait_send()


def reduce_owners(partial, toa_devices):
    pulsars, height, columns = partial.shape
    owned = pulsars // toa_devices
    chips = toa_devices // 2
    moved = owned * (chips - 1)
    block = (height, columns)
    return pl.pallas_call(
        functools.partial(reduce_kernel, chips),
        out_shape=jax.ShapeDtypeStruct((owned,) + block, jnp.float32),
        in_specs=[pl.BlockSpec(memory_space=pltpu.VMEM)],
        out_specs=pl.BlockSpec(memory_space=pltpu.VMEM),
        scratch_shapes=[
            pltpu.VMEM((owned * chips,) + block, jnp.float32),
            pltpu.VMEM((moved,) + block, jnp.float32),
            pltpu.VMEM((moved,) + block, jnp.float32),
            pltpu.SemaphoreType.DMA((owned * chips,)),
            pltpu.SemaphoreType.DMA((owned * chips,)),
            pltpu.SemaphoreType.DMA((moved,)),
            pltpu.SemaphoreType.DMA((moved,)),
        ],
        compiler_params=pltpu.CompilerParams(collective_id=0, has_side_effects=True),
        cost_estimate=pl.CostEstimate(flops=4 * pulsars * height * columns, bytes_accessed=40 * pulsars * height * columns, transcendentals=0),
        name="reduce_owners",
    )(partial)


def gather_kernel(groups, chips, mine_ref, out_ref, all_ref, psr_send, chip_send, core_send, recv):
    psr, me = lax.axis_index("psr"), lax.axis_index("toa")
    toa_devices = 2 * chips
    core = lax.rem(me, 2)
    chip = me // 2
    other = 1 - core
    partner = chip * 2 + other
    barrier = pltpu.get_barrier_semaphore()

    def greet(psr_to, toa_to):
        pl.semaphore_signal(barrier, inc=1, device_id={"psr": psr_to, "toa": toa_to}, device_id_type=MESH)

    greet(psr, partner)
    for d in range(1, chips):
        greet(psr, lax.rem(chip + d, chips) * 2 + core)
    for e in range(1, groups):
        greet(lax.rem(psr + e, groups), me)
    pl.semaphore_wait(barrier, chips + groups - 1)
    sent = []

    def block_of(e, toa):
        return lax.rem(psr + groups - e, groups) * toa_devices + toa

    def copy(source, block, sem, psr_to, toa_to):
        return pltpu.make_async_remote_copy(
            src_ref=source,
            dst_ref=all_ref.at[block],
            send_sem=sem,
            recv_sem=recv.at[block],
            device_id={"psr": psr_to, "toa": toa_to},
            device_id_type=MESH,
        )

    def send(source, block, sem, psr_to, toa_to):
        moving = copy(source, block, sem, psr_to, toa_to)
        moving.start()
        sent.append(moving)

    def arrived(block):
        copy(all_ref.at[block], block, core_send.at[0], psr, partner).wait_recv()

    own = psr * toa_devices + me
    for e in range(1, groups):
        send(mine_ref, own, psr_send.at[e - 1], lax.rem(psr + e, groups), me)
    for e in range(groups):
        block = block_of(e, me)
        if e:
            arrived(block)
        source = all_ref.at[block] if e else mine_ref
        for d in range(1, chips):
            send(source, block, chip_send.at[e * (chips - 1) + d - 1], psr, lax.rem(chip + d, chips) * 2 + core)
        send(source, block, core_send.at[e], psr, partner)
    for d in range(1, chips):
        for e in range(groups):
            block = block_of(e, lax.rem(chip + chips - d, chips) * 2 + core)
            arrived(block)
            send(all_ref.at[block], block, core_send.at[d * groups + e], psr, partner)
    all_ref[own] = mine_ref[...]
    for c in range(chips):
        for e in range(groups):
            arrived(block_of(e, c * 2 + other))
    for moving in sent:
        moving.wait_send()
    out_ref[...] = all_ref[...]


def gather_all(mine, groups, toa_devices):
    chips = toa_devices // 2
    devices = groups * toa_devices
    return pl.pallas_call(
        functools.partial(gather_kernel, groups, chips),
        out_shape=jax.ShapeDtypeStruct((devices,) + mine.shape, jnp.float32),
        in_specs=[pl.BlockSpec(memory_space=pltpu.VMEM)],
        out_specs=pl.BlockSpec(memory_space=pltpu.VMEM),
        scratch_shapes=[
            pltpu.VMEM((devices,) + mine.shape, jnp.float32),
            pltpu.SemaphoreType.DMA((groups - 1,)),
            pltpu.SemaphoreType.DMA((groups * (chips - 1),)),
            pltpu.SemaphoreType.DMA((groups * chips,)),
            pltpu.SemaphoreType.DMA((devices,)),
        ],
        compiler_params=pltpu.CompilerParams(collective_id=1, has_side_effects=True),
        name="gather_all",
    )(mine)


def body(design, noise_weight, residuals, slot_pulsar, slot_rows, own_prior, spectrum, directions):
    toa_devices = lax.axis_size("toa")
    owned = GROUP_PULSARS // toa_devices
    device = lax.axis_index("psr") * toa_devices + lax.axis_index("toa")
    partial = local_grams(design, noise_weight, residuals, slot_pulsar, slot_rows)
    sums = reduce_owners(partial, toa_devices)
    coupling = coupling_inverse(directions)
    power = 1.0 / jnp.repeat(spectrum, 2)
    packed, extra = eliminate(sums, own_prior, coupling, power[None, :], toa_devices)
    mine = packed.reshape(-1, packed.shape[-1])
    everything = gather_all(mine, lax.axis_size("psr"), toa_devices)
    whole = conjugate(everything, coupling, power[:, None])
    common = whole.shape[1]
    solution = lax.dynamic_slice_in_dim(whole, device * owned, owned, 0)
    chi_square = (extra[:, common + 1] - jnp.sum(extra[:, :common] * solution, axis=1)) / extra[:, common + 2]
    return (solution, extra[:, common], chi_square)


def solution(mesh):
    return jax.shard_map(
        body,
        mesh=mesh,
        in_specs=(
            P(("psr", "toa"), None, None),
            P(("psr", "toa"), None),
            P(("psr", "toa"), None),
            P(("psr", "toa")),
            P(("psr", "toa")),
            P(("psr", "toa"), None),
            P(),
            P(),
        ),
        out_specs=(P(("psr", "toa"), None), P(("psr", "toa")), P(("psr", "toa"))),
        check_vma=False,
    )
```
